32 devices in a mesh: lat: 4 (over z), rad: 8 (over y, x, core).
Axes of the slice: x: 2, y: 2, z: 4, core: 2. Of those that a mesh axis runs over, the one named last changes fastest.
Arguments:
- positions: float32 [4096, 3, 128], P(('lat', 'rad')), may hold values from 0 to 1
- fields: bfloat16 [4096, 16, 128], P(('lat', 'rad')), may hold values from -6 to 6
- velocity: float32 [81, 8192], P(None, ('lat', 'rad')), may hold values from -3 to 3
- counts: int32 [32], P(('lat', 'rad')), may hold values from 1 to 128, as said below
- elements: int32 [3, 4096], P(None, ('lat', 'rad')), may hold values from 0 to 255
- routes: int32 [2, 4096], P(None, ('lat', 'rad')), may hold values from 0 to 239, as said below
Outputs:
- moved: float32 [7680, 3, 128], P(('lat', 'rad'))
- projected: float32 [27, 16, 8192], P(None, None, ('lat', 'rad'))
The draws below stay inside these ranges and needn't reach their ends.
Inputs may be any that keep to these rules, and one draw needn't show every extreme that they name: counts[d] is at most 128 and equals 128 on some device. Both rows code destinations as in the reference program. routes[0] differs between any two blocks of one device; routes[1] differs between any two blocks that routes[0] sends to the same device.
All inputs are finite; a program needn't handle non-finite values.
Results may differ from the reference program's by a relative error of at most 0.0003.
Values sent between devices are 32-bit elements; how exact they have to be, the bound alone decides.
No kernel may reach another device: no remote copies, remote signals or barrier semaphores. Data moves between devices by JAX's collectives and lax.ppermute only.
A program may use at most 64 MiB of HBM per device.

```python
import jax
import jax.numpy as jnp
from jax import lax

BLOCK = 128
FIELDS = 16
MB = 128
NE = 256
CAP = 10
SLOTS = 240
BLOCKS = 4096
ELEMS = 8192
N_LAT = 4
N_RAD = 8
DEVICES = 32


def draw_counts(key, part):
    keys = jax.random.split(jax.random.fold_in(key, 11), 2)
    lowest = max(1, MB // 4)
    drawn = jax.random.randint(keys[0], (DEVICES,), lowest, MB + 1)
    fullest = jax.random.randint(keys[1], (), 0, DEVICES)
    return jnp.where(jnp.arange(DEVICES) == fullest, MB, drawn).astype(jnp.int32)


def shuffled(key, height, width):
    scores = jax.random.randint(key, (height, width), 0, 1 << 20) * width + jnp.arange(width)[None, :]
    return jnp.argsort(scores, axis=1).astype(jnp.int32)


def draw_routes(key, part):
    keys = jax.random.split(jax.random.fold_in(key, 23), 2)
    first_route = shuffled(keys[0], DEVICES, SLOTS)[:, :MB].reshape(-1)
    home = jnp.arange(DEVICES * MB, dtype=jnp.int32) // MB
    lat_step = first_route // (N_RAD * CAP)
    mid_rad = first_route // CAP % N_RAD
    mid_place = first_route % CAP
    middle = (home // N_RAD + lat_step - 1) % N_LAT * N_RAD + mid_rad
    arrival = (lat_step * N_RAD + home % N_RAD) * CAP + mid_place
    second_route = shuffled(keys[1], DEVICES, SLOTS)[middle, arrival]
    return jnp.stack([first_route, second_route]).astype(jnp.int32)


def set_ends(result, key, smallest, top_value):
    place = [jax.random.randint(jax.random.fold_in(key, axis), (), 0, length) for axis, length in enumerate(result.shape)]
    longest = result.shape.index(max(result.shape))
    next_to = place[:longest] + [(place[longest] + 1) % result.shape[longest]] + place[longest + 1:]
    return result.at[tuple(place)].set(smallest).at[tuple(next_to)].set(top_value)


def block_levels(key, shape, cuts, least, top_value):
    loudness = 1.0
    for position, blocks in cuts:
        steps = jax.random.uniform(jax.random.fold_in(jax.random.fold_in(key, 6), position), (blocks,), jnp.float32, least / len(cuts), top_value / len(cuts))
        loudness = loudness * jnp.repeat(jnp.exp(steps), shape[position] // blocks).reshape((-1,) + (1,) * (len(shape) - 1 - position))
    return loudness


def bell_draw(rng, dims, deviation, limit, pieces=(), kind=jnp.bfloat16):
    result = deviation * jax.random.normal(rng, dims, jnp.float32)
    if pieces:
        result = result * block_levels(rng, dims, pieces, -0.22, 0.18)
    return jnp.clip(result, -limit, limit).astype(kind)


def setup_inputs(seed: int = 0) -> dict:
    seeds = jax.random.split(jax.random.key(seed), 7)
    return {
        "positions": jnp.clip(1.0 * jax.random.uniform(seeds[0], (BLOCKS, 3, BLOCK), jnp.float32) ** block_levels(seeds[0], (BLOCKS, 3, BLOCK), ((0, 32),), -0.2, 0.2), 0.0, 1.0),
        "fields": bell_draw(seeds[1], (BLOCKS, FIELDS, BLOCK), 1.0, 6.0, ((0, 32),)),
        "velocity": bell_draw(seeds[2], (81, ELEMS), 0.5, 3.0, ((1, 32),), jnp.float32),
        "counts": draw_counts(jax.random.fold_in(seeds[6], 71), 0),
        "elements": set_ends(jax.random.randint(seeds[4], (3, BLOCKS), 0, NE), jax.random.fold_in(seeds[4], 1), 0, NE - 1).astype(jnp.int32),
        "routes": draw_routes(jax.random.fold_in(seeds[6], 71), 0),
    }


time_step = 0.4
exact = lax.Precision.HIGHEST


def lagrange(coord):
    first_node = 2.0 * (coord - 0.5) * (coord - 1.0)
    middle_node = -4.0 * coord * (coord - 1.0)
    last_node = 2.0 * coord * (coord - 0.5)
    return jnp.stack([first_node, middle_node, last_node], axis=0)


def basis(points):
    along_x = lagrange(points[:, 0, :])
    along_y = lagrange(points[:, 1, :])
    along_z = lagrange(points[:, 2, :])
    table = along_x[:, None, None] * along_y[None, :, None] * along_z[None, None, :]
    return jnp.moveaxis(table.reshape(27, points.shape[0], points.shape[2]), 0, 1)


def speed(columns, points):
    coefficients = columns.T.reshape(points.shape[0], 3, 27)
    return jnp.einsum("scn,snb->scb", coefficients, basis(points), precision=exact)


def reference(positions, fields, velocity, counts, elements, routes):
    devices = N_LAT * N_RAD
    total = positions.shape[0]
    width = positions.shape[2]
    order = jnp.arange(total, dtype=jnp.int32)
    home = order // MB
    valid = (order % MB) < counts[home]
    lat_step = routes[0] // (N_RAD * CAP)
    mid_rad = (routes[0] // CAP) % N_RAD
    mid_lat = (home // N_RAD + lat_step - 1) % N_LAT
    middle = mid_lat * N_RAD + mid_rad
    next_step = routes[1] // (N_RAD * CAP)
    final_rad = (routes[1] // CAP) % N_RAD
    final_place = routes[1] % CAP
    final = ((mid_lat + next_step - 1) % N_LAT) * N_RAD + final_rad
    out_rows = (final * SLOTS + (next_step * N_RAD + mid_rad) * CAP + final_place).astype(jnp.int32)
    start_cols = (home * NE + elements[0]).astype(jnp.int32)
    middle_cols = (middle * NE + elements[1]).astype(jnp.int32)
    final_cols = (final * NE + elements[2]).astype(jnp.int32)

    def advance(block_set):
        points, fractions, start, middle_col = block_set
        first_speed = speed(jnp.take(velocity, start, axis=1), points)
        midway = points + (0.5 * time_step) * first_speed
        landed = points + time_step * speed(jnp.take(velocity, middle_col, axis=1), midway)
        shapes = basis(landed)
        moments = jnp.einsum("snb,sfb->snf", shapes, fractions.astype(jnp.float32), precision=exact)
        return landed, moments, jnp.sum(shapes * shapes, axis=2)

    landed, moments, weights = lax.map(advance, (positions.reshape(devices, MB, 3, width), fields.reshape(devices, MB, fields.shape[1], width), start_cols.reshape(devices, MB), middle_cols.reshape(devices, MB)))
    landed = landed.reshape(total, 3, width)
    moments = moments.reshape(total, 27, fields.shape[1])
    weights = weights.reshape(total, 27)
    live = valid.astype(jnp.float32)
    moved = jnp.zeros((devices * SLOTS, 3, width), jnp.float32).at[out_rows].set(landed * live[:, None, None])
    totals = jax.ops.segment_sum(moments * live[:, None, None], final_cols, num_segments=devices * NE)
    summed = jax.ops.segment_sum(weights * live[:, None], final_cols, num_segments=devices * NE)
    projected = totals / (1.0 + summed[:, :, None])
    return moved, jnp.transpose(projected, (1, 2, 0))
```

```python
import jax
import jax.numpy as jnp
import numpy as np
from jax import lax
from jax.experimental import pallas as pl
from jax.experimental.pallas import tpu as pltpu
from jax.sharding import PartitionSpec as P

time_step = 0.4
exact = lax.Precision.HIGHEST
LANES = 128
VM = pl.BlockSpec(memory_space=pltpu.VMEM)
SM = pl.BlockSpec(memory_space=pltpu.SMEM)
f32 = jnp.float32
bf16 = jnp.bfloat16


def passed_along(x, axis, by):
    size = lax.axis_size(axis)
    return lax.ppermute(x, axis, [(i, (i + by) % size) for i in range(size)])


def lagrange(coord):
    return (
        2.0 * (coord - 0.5) * (coord - 1.0),
        -4.0 * coord * (coord - 1.0),
        2.0 * coord * (coord - 0.5),
    )


def columns_of(velocity, picks):
    owned = velocity.shape[1]
    table = jnp.pad(velocity, ((0, LANES - velocity.shape[0]), (0, 0)))
    chosen = (picks[:, None] == jnp.arange(owned, dtype=jnp.int32)[None, :]).astype(f32)
    return lax.dot_general(chosen, table, (((1,), (1,)), ((), ())), precision=exact)


def eight_speeds(columns, x, y, z):
    lx, ly, lz = lagrange(x), lagrange(y), lagrange(z)
    out = []
    for c in range(3):
        total = None
        for i in range(3):
            plane = None
            for j in range(3):
                base = c * 27 + i * 9 + j * 3
                line = sum(columns[:, base + k : base + k + 1] * lz[k] for k in range(3))
                line = line * ly[j]
                plane = line if plane is None else plane + line
            plane = plane * lx[i]
            total = plane if total is None else total + plane
        out.append(total)
    return out


def midway_kernel(pos_ref, col_ref, out_ref):
    def group(g, carry):
        rows = pl.ds(pl.multiple_of(g * 8, 8), 8)
        x, y, z = (pos_ref[c, rows, :] for c in range(3))
        u = eight_speeds(col_ref[rows, :], x, y, z)
        for c, p in enumerate((x, y, z)):
            out_ref[c, rows, :] = p + (0.5 * time_step) * u[c]
        return carry

    lax.fori_loop(0, pos_ref.shape[1] // 8, group, 0)


def home_kernel(row_ref, src_ref, e2_ref, pos_ref, mid_ref, reply_ref, fields_ref, const_ref,
                out0, out1, out2, cols, land, tiles):
    blocks = pos_ref.shape[1]

    def fetch(g, carry):
        for i in range(8):
            s = g * 8 + i
            cols[pl.ds(s, 1), :] = reply_ref[pl.ds(row_ref[s], 1), :]
        return carry

    lax.fori_loop(0, blocks // 8, fetch, 0)

    def group(g, carry):
        rows = pl.ds(pl.multiple_of(g * 8, 8), 8)
        x, y, z = (mid_ref[c, rows, :] for c in range(3))
        u = eight_speeds(cols[rows, :], x, y, z)
        for c in range(3):
            land[c, rows, :] = pos_ref[c, rows, :] + time_step * u[c]
        return carry

    lax.fori_loop(0, blocks // 8, group, 0)

    lane = lax.broadcasted_iota(jnp.int32, (8, LANES), 1)
    sub = lax.broadcasted_iota(jnp.int32, (8, LANES), 0)
    own_slot = (lane // 16) == sub

    def block(g, carry):
        for i in range(8):
            s = g * 8 + i
            coords = [land[c, pl.ds(s, 1), :] for c in range(3)]
            phi = const_ref[6]
            for c in range(3):
                phi = phi * ((coords[c] - const_ref[2 * c]) * (coords[c] - const_ref[2 * c + 1]))
            high = phi.astype(bf16)
            low = (phi - high.astype(f32)).astype(bf16)
            spread = jnp.concatenate([fields_ref[s]] * 8, axis=0)
            dims = (((1,), (1,)), ((), ()))
            both = lax.dot_general(jnp.concatenate([high, low], axis=0), spread, dims,
                                   preferred_element_type=f32)
            full = both[:32] + both[32:]
            rows = list(coords)
            for j in range(4):
                rows.append(jnp.sum(jnp.where(own_slot, full[8 * j : 8 * j + 8], 0.0), axis=0, keepdims=True))
            weight = jnp.sum(phi * phi, axis=1, keepdims=True)
            tag = (e2_ref[s] + 1).astype(f32)
            last = jnp.where((lane == 32) & (sub == 0), tag, 0.0)
            for j in range(4):
                last = last + jnp.where(lane == sub + 8 * j, weight[8 * j : 8 * j + 8], 0.0)
            rows.append(jnp.sum(last, axis=0, keepdims=True))
            tiles[s] = jnp.concatenate(rows, axis=0)
        return carry

    lax.fori_loop(0, blocks // 8, block, 0)
    tiles[blocks] = jnp.zeros((8, LANES), f32)
    send(src_ref, tiles, (out0, out1, out2))


def send(src_ref, tiles, outs):
    count = outs[0].shape[0]
    step = next(s for s in (8, 4, 2, 1) if count % s == 0)
    for k, out in enumerate(outs):
        def some(g, carry):
            for i in range(step):
                p = g * step + i
                out[p] = tiles[src_ref[k * count + p]]
            return carry

        lax.fori_loop(0, count // step, some, 0)


def middle_kernel(src_ref, in0, in1, in2, out0, out1, out2, tiles):
    count = in0.shape[0]
    for k, ref in enumerate((in0, in1, in2)):
        tiles[k * count : (k + 1) * count] = ref[...]
    tiles[3 * count] = jnp.zeros((8, LANES), f32)
    send(src_ref, tiles, (out0, out1, out2))


def final_kernel(in0, in1, in2, moved_ref, proj_ref):
    count = in0.shape[0]
    owned = proj_ref.shape[2]
    fields = proj_ref.shape[1]
    for k, ref in enumerate((in0, in1, in2)):
        moved_ref[k * count : (k + 1) * count] = ref[:, 0:3, :]

    def row(j):
        return jnp.concatenate([ref[:, j, :] for ref in (in0, in1, in2)], axis=0)

    last = row(7)
    tag = last[:, 32:33].astype(jnp.int32) - 1
    hits = (tag == lax.broadcasted_iota(jnp.int32, (3 * count, owned), 1)).astype(bf16)
    dims = (((0,), (0,)), ((), ()))

    def summed(x):
        high = x.astype(bf16)
        low = (x - high.astype(f32)).astype(bf16)
        return (lax.dot_general(high, hits, dims, preferred_element_type=f32)
                + lax.dot_general(low, hits, dims, preferred_element_type=f32))

    scale = 1.0 / (1.0 + summed(last))
    for j in range(4):
        total = summed(row(3 + j))
        for i in range(8):
            n = 8 * j + i
            if n < proj_ref.shape[0]:
                proj_ref[n] = total[fields * i : fields * (i + 1)] * scale[n : n + 1]


def node_constants():
    roots = ((0.5, 1.0, 2.0), (0.0, 1.0, -4.0), (0.0, 0.5, 2.0))
    table = np.zeros((7, 32, LANES), np.float32)
    for n in range(27):
        table[6, n] = 1.0
        for c, i in enumerate((n // 9, n // 3 % 3, n % 3)):
            table[2 * c, n], table[2 * c + 1, n] = roots[i][0], roots[i][1]
            table[6, n] *= roots[i][2]
    return table


def hop(sheets):
    arrived = []
    for k in (0, 2, 1):
        sheet = lax.all_to_all(sheets[k], "rad", split_axis=0, concat_axis=0, tiled=True)
        if k != 1:
            sheet = passed_along(sheet, "lat", k - 1)
        arrived.append(sheet)
    return arrived[0], arrived[2], arrived[1]


def per_device(positions, fields, velocity, counts, elements, routes):
    lat_count, rad_count = lax.axis_size("lat"), lax.axis_size("rad")
    lat = lax.axis_index("lat")
    devices = lat_count * rad_count
    blocks = positions.shape[0]
    capacity = max(1, 2 * blocks // (3 * rad_count))
    sheet = rad_count * capacity
    places = 3 * sheet
    order = jnp.arange(blocks, dtype=jnp.int32)
    valid = order < counts[0]
    lat_to = (lat + routes[0] // sheet - 1) % lat_count
    row_of = (lat_to * sheet + routes[0] % sheet).astype(jnp.int32)

    at_row = (row_of[None, :] == jnp.arange(devices * capacity, dtype=jnp.int32)[:, None]) & valid[None, :]
    want = jnp.max(jnp.where(at_row, elements[1][None, :], -1), axis=1)
    route = jnp.max(jnp.where(at_row, routes[1][None, :], -1), axis=1)
    request = jnp.concatenate([want.reshape(devices, capacity), route.reshape(devices, capacity)], axis=1)
    request = lax.all_to_all(request, ("lat", "rad"), split_axis=0, concat_axis=0, tiled=True)
    asked, next_route = request[:, :capacity].reshape(-1), request[:, capacity:].reshape(-1)
    reply = columns_of(velocity, asked).reshape(devices, capacity, LANES)
    reply = lax.all_to_all(reply, ("lat", "rad"), split_axis=0, concat_axis=0, tiled=True)
    reply = reply.reshape(devices * capacity, LANES)

    place = jnp.arange(places, dtype=jnp.int32)
    at_place = (routes[0][None, :] == place[:, None]) & valid[None, :]
    first_source = jnp.min(jnp.where(at_place, order[None, :], blocks), axis=1)
    came = jnp.arange(devices * capacity, dtype=jnp.int32)
    sheet_in = (lat - came // sheet + 1) % lat_count
    index_in = sheet_in * sheet + came % sheet
    at_place = next_route[None, :] == place[:, None]
    second_source = jnp.min(jnp.where(at_place, index_in[None, :], places), axis=1)

    points = jnp.transpose(positions, (1, 0, 2))
    midway = pl.pallas_call(
        midway_kernel, out_shape=jax.ShapeDtypeStruct(points.shape, f32),
        in_specs=[VM, VM], out_specs=VM, name="midway",
    )(points, columns_of(velocity, elements[0]))

    part = jax.ShapeDtypeStruct((sheet, 8, LANES), f32)
    sheets = pl.pallas_call(
        home_kernel, out_shape=[part] * 3,
        in_specs=[SM] * 3 + [VM] * 5, out_specs=[VM] * 3, name="home",
        scratch_shapes=[pltpu.VMEM((blocks, LANES), f32), pltpu.VMEM((3, blocks, LANES), f32),
                        pltpu.VMEM((blocks + 1, 8, LANES), f32)],
    )(row_of, first_source, elements[2], points, midway, reply, fields, jnp.asarray(node_constants()))
    sheets = hop(sheets)
    sheets = pl.pallas_call(
        middle_kernel, out_shape=[part] * 3,
        in_specs=[SM] + [VM] * 3, out_specs=[VM] * 3, name="middle",
        scratch_shapes=[pltpu.VMEM((places + 1, 8, LANES), f32)],
    )(second_source, *sheets)
    sheets = hop(sheets)
    return pl.pallas_call(
        final_kernel,
        out_shape=[jax.ShapeDtypeStruct((places,) + positions.shape[1:], f32),
                   jax.ShapeDtypeStruct((27, fields.shape[1], velocity.shape[1]), f32)],
        in_specs=[VM] * 3, out_specs=[VM] * 2, name="final",
    )(*sheets)


def solution(mesh):
    in_specs = (
        P(("lat", "rad"), None, None),
        P(("lat", "rad"), None, None),
        P(None, ("lat", "rad")),
        P(("lat", "rad")),
        P(None, ("lat", "rad")),
        P(None, ("lat", "rad")),
    )
    out_specs = (P(("lat", "rad"), None, None), P(None, None, ("lat", "rad")))

    def body(*args):
        return tuple(per_device(*args))

    return jax.shard_map(
        body, mesh=mesh, in_specs=in_specs, out_specs=out_specs, check_vma=False
    )
```

```python
from functools import partial

import jax
import jax.numpy as jnp
import numpy as np
from jax import lax
from jax.experimental import pallas as pl
from jax.experimental.pallas import tpu as pltpu
from jax.sharding import PartitionSpec as P

time_step = 0.4
exact = lax.Precision.HIGHEST
LANES = 128
ROWS = 7
TAG = 80
VM = pl.BlockSpec(memory_space=pltpu.VMEM)
SM = pl.BlockSpec(memory_space=pltpu.SMEM)
f32 = jnp.float32
bf16 = jnp.bfloat16


def passed_along(x, axis, by):
    size = lax.axis_size(axis)
    return lax.ppermute(x, axis, [(i, (i + by) % size) for i in range(size)])


def lagrange(coord):
    return (
        2.0 * (coord - 0.5) * (coord - 1.0),
        -4.0 * coord * (coord - 1.0),
        2.0 * coord * (coord - 0.5),
    )


def columns_of(velocity, picks):
    owned = velocity.shape[1]
    table = jnp.pad(velocity, ((0, LANES - velocity.shape[0]), (0, 0)))
    chosen = (picks[:, None] == jnp.arange(owned, dtype=jnp.int32)[None, :]).astype(f32)
    return lax.dot_general(chosen, table, (((1,), (1,)), ((), ())), precision=exact)


def eight_speeds(columns, x, y, z):
    lx, ly, lz = lagrange(x), lagrange(y), lagrange(z)
    out = []
    for c in range(3):
        total = None
        for i in range(3):
            plane = None
            for j in range(3):
                base = c * 27 + i * 9 + j * 3
                line = sum(columns[:, base + k : base + k + 1] * lz[k] for k in range(3))
                line = line * ly[j]
                plane = line if plane is None else plane + line
            plane = plane * lx[i]
            total = plane if total is None else total + plane
        out.append(total)
    return out


def midway_kernel(pos_ref, col_ref, out_ref):
    for g in range(pos_ref.shape[1] // 8):
        rows = slice(g * 8, g * 8 + 8)
        x, y, z = (pos_ref[c, rows, :] for c in range(3))
        u = eight_speeds(col_ref[rows, :], x, y, z)
        for c, p in enumerate((x, y, z)):
            out_ref[c, rows, :] = p + (0.5 * time_step) * u[c]


def home_kernel(row_ref, src_ref, e2_ref, pos_ref, mid_ref, reply_ref, fields_ref, const_ref,
                side, straight, cols, land, tiles, *, capacity):
    blocks = pos_ref.shape[1]

    def fetch(g, carry):
        for i in range(8):
            s = g * 8 + i
            cols[pl.ds(s, 1), :] = reply_ref[pl.ds(row_ref[s], 1), :]
        return carry

    lax.fori_loop(0, blocks // 8, fetch, 0)

    for g in range(blocks // 8):
        rows = slice(g * 8, g * 8 + 8)
        x, y, z = (mid_ref[c, rows, :] for c in range(3))
        u = eight_speeds(cols[rows, :], x, y, z)
        for c in range(3):
            land[c, rows, :] = pos_ref[c, rows, :] + time_step * u[c]

    lane = lax.broadcasted_iota(jnp.int32, (8, LANES), 1)
    sub = lax.broadcasted_iota(jnp.int32, (8, LANES), 0)
    own_slot = (lane // 16) == sub
    tag_slot = (lane == TAG) & (sub == 0)

    def block(g, carry):
        for i in range(8):
            s = g * 8 + i
            coords = [land[c, pl.ds(s, 1), :] for c in range(3)]
            phi = const_ref[6]
            for c in range(3):
                phi = phi * ((coords[c] - const_ref[2 * c]) * (coords[c] - const_ref[2 * c + 1]))
            high = phi.astype(bf16)
            low = (phi - high.astype(f32)).astype(bf16)
            spread = jnp.concatenate([fields_ref[s]] * 8, axis=0)
            dims = (((1,), (1,)), ((), ()))
            both = lax.dot_general(jnp.concatenate([high, low], axis=0), spread, dims,
                                   preferred_element_type=f32)
            full = both[:32] + both[32:]
            weight = jnp.sum(phi * phi, axis=1, keepdims=True)
            tag = (e2_ref[s] + 1).astype(f32)
            parts = [jnp.where(own_slot, full[8 * j : 8 * j + 8], 0.0) for j in range(4)]
            parts[3] = jnp.where(tag_slot, tag, parts[3])
            for j in range(4):
                parts[3] = jnp.where(lane == sub + (48 + 8 * j), weight[8 * j : 8 * j + 8], parts[3])
            rows = coords + [jnp.sum(part, axis=0, keepdims=True) for part in parts]
            tiles[s, 0:7, :] = jnp.concatenate(rows, axis=0)
        return carry

    lax.fori_loop(0, blocks // 8, block, 0)
    tiles[blocks] = jnp.zeros((8, LANES), f32)
    send(src_ref, tiles, side, straight, capacity)


def send(src_ref, tiles, side, straight, capacity):
    rad_count = straight.shape[0]

    def some(q, carry):
        for k in range(3):
            for c in range(capacity):
                tile = tiles[src_ref[(k * rad_count + q) * capacity + c], 0:ROWS, :]
                rows = slice(c * ROWS, (c + 1) * ROWS)
                if k == 1:
                    straight[q, rows, :] = tile
                else:
                    side[q, k // 2, rows, :] = tile
        return carry

    lax.fori_loop(0, rad_count, some, 0)


def collect(ins, tiles, capacity):
    rad_count = ins[0].shape[0]

    def some(q, carry):
        for k, ref in enumerate(ins):
            for c in range(capacity):
                p = (k * rad_count + q) * capacity + c
                tiles[p, 0:ROWS, :] = ref[q, c * ROWS : (c + 1) * ROWS, :]
        return carry

    lax.fori_loop(0, rad_count, some, 0)


def middle_kernel(src_ref, in0, in1, in2, side, straight, tiles, *, capacity):
    collect((in0, in1, in2), tiles, capacity)
    tiles[tiles.shape[0] - 1] = jnp.zeros((8, LANES), f32)
    send(src_ref, tiles, side, straight, capacity)


def final_kernel(in0, in1, in2, moved_ref, proj_ref, tiles, *, capacity):
    places = tiles.shape[0]
    owned = proj_ref.shape[2]
    fields = proj_ref.shape[1]
    collect((in0, in1, in2), tiles, capacity)
    moved_ref[...] = tiles[:, 0:3, :]

    def row(j):
        return tiles[:, j, :]

    last = row(6)
    tag = last[:, TAG : TAG + 1].astype(jnp.int32) - 1
    hits = (tag == lax.broadcasted_iota(jnp.int32, (places, owned), 1)).astype(bf16)
    dims = (((0,), (0,)), ((), ()))

    def summed(x):
        high = x.astype(bf16)
        low = (x - high.astype(f32)).astype(bf16)
        return (lax.dot_general(high, hits, dims, preferred_element_type=f32)
                + lax.dot_general(low, hits, dims, preferred_element_type=f32))

    total = summed(last)
    scale = 1.0 / (1.0 + total[48:80])
    for j in (3, 0, 1, 2):
        if j < 3:
            total = summed(row(3 + j))
        for i in range(8):
            n = 8 * j + i
            if n < proj_ref.shape[0]:
                proj_ref[n] = total[fields * i : fields * (i + 1)] * scale[n : n + 1]


def node_constants():
    roots = ((0.5, 1.0, 2.0), (0.0, 1.0, -4.0), (0.0, 0.5, 2.0))
    table = np.zeros((7, 32, LANES), np.float32)
    for n in range(27):
        table[6, n] = 1.0
        for c, i in enumerate((n // 9, n // 3 % 3, n % 3)):
            table[2 * c, n], table[2 * c + 1, n] = roots[i][0], roots[i][1]
            table[6, n] *= roots[i][2]
    return table


def hop(side, straight):
    side = lax.all_to_all(side, "rad", split_axis=0, concat_axis=0, tiled=True)
    back = passed_along(side[:, 0], "lat", -1)
    onward = passed_along(side[:, 1], "lat", 1)
    straight = lax.all_to_all(straight, "rad", split_axis=0, concat_axis=0, tiled=True)
    return back, straight, onward


def per_device(positions, fields, velocity, counts, elements, routes):
    lat_count, rad_count = lax.axis_size("lat"), lax.axis_size("rad")
    lat = lax.axis_index("lat")
    devices = lat_count * rad_count
    blocks = positions.shape[0]
    capacity = max(1, 2 * blocks // (3 * rad_count))
    sheet = rad_count * capacity
    places = 3 * sheet
    order = jnp.arange(blocks, dtype=jnp.int32)
    valid = order < counts[0]
    lat_to = (lat + routes[0] // sheet - 1) % lat_count
    row_of = (lat_to * sheet + routes[0] % sheet).astype(jnp.int32)

    at_row = (row_of[None, :] == jnp.arange(devices * capacity, dtype=jnp.int32)[:, None]) & valid[None, :]
    want = jnp.max(jnp.where(at_row, elements[1][None, :], -1), axis=1)
    route = jnp.max(jnp.where(at_row, routes[1][None, :], -1), axis=1)
    request = jnp.concatenate([want.reshape(devices, capacity), route.reshape(devices, capacity)], axis=1)
    request = lax.all_to_all(request, ("lat", "rad"), split_axis=0, concat_axis=0, tiled=True)
    asked, next_route = request[:, :capacity].reshape(-1), request[:, capacity:].reshape(-1)
    reply = columns_of(velocity, asked).reshape(devices, capacity, LANES)
    reply = lax.all_to_all(reply, ("lat", "rad"), split_axis=0, concat_axis=0, tiled=True)
    reply = reply.reshape(devices * capacity, LANES)

    place = jnp.arange(places, dtype=jnp.int32)
    at_place = (routes[0][None, :] == place[:, None]) & valid[None, :]
    first_source = jnp.min(jnp.where(at_place, order[None, :], blocks), axis=1)
    came = jnp.arange(devices * capacity, dtype=jnp.int32)
    sheet_in = (lat - came // sheet + 1) % lat_count
    index_in = sheet_in * sheet + came % sheet
    at_place = next_route[None, :] == place[:, None]
    second_source = jnp.min(jnp.where(at_place, index_in[None, :], places), axis=1)

    points = jnp.transpose(positions, (1, 0, 2))
    midway = pl.pallas_call(
        midway_kernel, out_shape=jax.ShapeDtypeStruct(points.shape, f32),
        in_specs=[VM, VM], out_specs=VM, name="midway",
    )(points, columns_of(velocity, elements[0]))

    group_rows = (ROWS * capacity + 7) // 8 * 8
    parcels = [jax.ShapeDtypeStruct((rad_count, 2, group_rows, LANES), f32),
               jax.ShapeDtypeStruct((rad_count, group_rows, LANES), f32)]
    parcels = pl.pallas_call(
        partial(home_kernel, capacity=capacity), out_shape=parcels,
        in_specs=[SM] * 3 + [VM] * 5, out_specs=[VM] * 2, name="home",
        scratch_shapes=[pltpu.VMEM((blocks, LANES), f32), pltpu.VMEM((3, blocks, LANES), f32),
                        pltpu.VMEM((blocks + 1, 8, LANES), f32)],
    )(row_of, first_source, elements[2], points, midway, reply, fields, jnp.asarray(node_constants()))
    parcels = pl.pallas_call(
        partial(middle_kernel, capacity=capacity),
        out_shape=[jax.ShapeDtypeStruct(x.shape, f32) for x in parcels],
        in_specs=[SM] + [VM] * 3, out_specs=[VM] * 2, name="middle",
        scratch_shapes=[pltpu.VMEM((places + 1, 8, LANES), f32)],
    )(second_source, *hop(*parcels))
    return pl.pallas_call(
        partial(final_kernel, capacity=capacity),
        out_shape=[jax.ShapeDtypeStruct((places,) + positions.shape[1:], f32),
                   jax.ShapeDtypeStruct((27, fields.shape[1], velocity.shape[1]), f32)],
        in_specs=[VM] * 3, out_specs=[VM] * 2, name="final",
        scratch_shapes=[pltpu.VMEM((places, 8, LANES), f32)],
    )(*hop(*parcels))


def solution(mesh):
    in_specs = (
        P(("lat", "rad"), None, None),
        P(("lat", "rad"), None, None),
        P(None, ("lat", "rad")),
        P(("lat", "rad")),
        P(None, ("lat", "rad")),
        P(None, ("lat", "rad")),
    )
    out_specs = (P(("lat", "rad"), None, None), P(None, None, ("lat", "rad")))

    def body(*args):
        return tuple(per_device(*args))

    return jax.shard_map(
        body, mesh=mesh, in_specs=in_specs, out_specs=out_specs, check_vma=False
    )
```

```python
from functools import partial

import jax
import jax.numpy as jnp
import numpy as np
from jax import lax
from jax.experimental import pallas as pl
from jax.experimental.pallas import tpu as pltpu
from jax.sharding import PartitionSpec as P

time_step = 0.4
exact = lax.Precision.HIGHEST
LANES = 128
ROWS = 7
TAG = 80
VM = pl.BlockSpec(memory_space=pltpu.VMEM)
SM = pl.BlockSpec(memory_space=pltpu.SMEM)
f32 = jnp.float32
bf16 = jnp.bfloat16


def passed_along(x, axis, by):
    size = lax.axis_size(axis)
    return lax.ppermute(x, axis, [(i, (i + by) % size) for i in range(size)])


def lagrange(coord):
    return (
        2.0 * (coord - 0.5) * (coord - 1.0),
        -4.0 * coord * (coord - 1.0),
        2.0 * coord * (coord - 0.5),
    )


def columns_of(velocity, picks):
    owned = velocity.shape[1]
    table = jnp.pad(velocity, ((0, LANES - velocity.shape[0]), (0, 0)))
    chosen = (picks[:, None] == jnp.arange(owned, dtype=jnp.int32)[None, :]).astype(f32)
    return lax.dot_general(chosen, table, (((1,), (1,)), ((), ())), precision=exact)


def eight_speeds(columns, x, y, z):
    lx, ly, lz = lagrange(x), lagrange(y), lagrange(z)
    out = []
    for c in range(3):
        total = None
        for i in range(3):
            plane = None
            for j in range(3):
                base = c * 27 + i * 9 + j * 3
                line = sum(columns[:, base + k : base + k + 1] * lz[k] for k in range(3))
                line = line * ly[j]
                plane = line if plane is None else plane + line
            plane = plane * lx[i]
            total = plane if total is None else total + plane
        out.append(total)
    return out


def midway_kernel(pos_ref, col_ref, out_ref):
    for g in range(pos_ref.shape[1] // 8):
        rows = slice(g * 8, g * 8 + 8)
        x, y, z = (pos_ref[c, rows, :] for c in range(3))
        u = eight_speeds(col_ref[rows, :], x, y, z)
        for c, p in enumerate((x, y, z)):
            out_ref[c, rows, :] = p + (0.5 * time_step) * u[c]


def home_kernel(row_ref, src_ref, e2_ref, pos_ref, mid_ref, reply_ref, fields_ref, const_ref,
                side, straight, cols, land, tiles, *, capacity):
    blocks = pos_ref.shape[1]

    def fetch(g, carry):
        for i in range(8):
            s = g * 8 + i
            cols[pl.ds(s, 1), :] = reply_ref[pl.ds(row_ref[s], 1), :]
        return carry

    lax.fori_loop(0, blocks // 8, fetch, 0)

    for g in range(blocks // 8):
        rows = slice(g * 8, g * 8 + 8)
        x, y, z = (mid_ref[c, rows, :] for c in range(3))
        u = eight_speeds(cols[rows, :], x, y, z)
        for c in range(3):
            land[c, rows, :] = pos_ref[c, rows, :] + time_step * u[c]

    lane = lax.broadcasted_iota(jnp.int32, (8, LANES), 1)
    sub = lax.broadcasted_iota(jnp.int32, (8, LANES), 0)
    own_slot = (lane // 16) == sub
    tag_slot = (lane == TAG) & (sub == 0)

    def block(g, carry):
        for i in range(8):
            s = g * 8 + i
            coords = [land[c, pl.ds(s, 1), :] for c in range(3)]
            phi = const_ref[6]
            for c in range(3):
                phi = phi * ((coords[c] - const_ref[2 * c]) * (coords[c] - const_ref[2 * c + 1]))
            high = phi.astype(bf16)
            low = (phi - high.astype(f32)).astype(bf16)
            spread = jnp.concatenate([fields_ref[s]] * 8, axis=0)
            dims = (((1,), (1,)), ((), ()))
            both = lax.dot_general(jnp.concatenate([high, low], axis=0), spread, dims,
                                   preferred_element_type=f32)
            full = both[:32] + both[32:]
            weight = jnp.sum(phi * phi, axis=1, keepdims=True)
            tag = (e2_ref[s] + 1).astype(f32)
            parts = [jnp.where(own_slot, full[8 * j : 8 * j + 8], 0.0) for j in range(4)]
            parts[3] = jnp.where(tag_slot, tag, parts[3])
            for j in range(4):
                parts[3] = jnp.where(lane == sub + (48 + 8 * j), weight[8 * j : 8 * j + 8], parts[3])
            rows = coords + [jnp.sum(part, axis=0, keepdims=True) for part in parts]
            tiles[s, 0:7, :] = jnp.concatenate(rows, axis=0)
        return carry

    lax.fori_loop(0, blocks // 8, block, 0)
    tiles[blocks] = jnp.zeros((8, LANES), f32)
    send(src_ref, tiles, side, straight, capacity)


def send(src_ref, tiles, side, straight, capacity):
    rad_count = straight.shape[0]

    def some(q, carry):
        for k in range(3):
            for c in range(capacity):
                tile = tiles[src_ref[(k * rad_count + q) * capacity + c], 0:ROWS, :]
                rows = slice(c * ROWS, (c + 1) * ROWS)
                if k == 1:
                    straight[q, rows, :] = tile
                else:
                    side[q, k // 2, rows, :] = tile
        return carry

    lax.fori_loop(0, rad_count, some, 0)


def collect(ins, tiles, capacity):
    rad_count = ins[0].shape[0]

    def some(q, carry):
        for k, ref in enumerate(ins):
            for c in range(capacity):
                p = (k * rad_count + q) * capacity + c
                tiles[p, 0:ROWS, :] = ref[q, c * ROWS : (c + 1) * ROWS, :]
        return carry

    lax.fori_loop(0, rad_count, some, 0)


def middle_kernel(src_ref, in0, in1, in2, side, straight, tiles, *, capacity):
    collect((in0, in1, in2), tiles, capacity)
    tiles[tiles.shape[0] - 1] = jnp.zeros((8, LANES), f32)
    send(src_ref, tiles, side, straight, capacity)


def final_kernel(in0, in1, in2, moved_ref, proj_ref, tiles, *, capacity):
    places = tiles.shape[0]
    owned = proj_ref.shape[2]
    fields = proj_ref.shape[1]
    collect((in0, in1, in2), tiles, capacity)
    for c in range(3):
        moved_ref[c] = tiles[:, c, :]

    def row(j):
        return tiles[:, j, :]

    last = row(6)
    tag = last[:, TAG : TAG + 1].astype(jnp.int32) - 1
    hits = (tag == lax.broadcasted_iota(jnp.int32, (places, owned), 1)).astype(bf16)
    dims = (((0,), (0,)), ((), ()))

    def summed(x):
        high = x.astype(bf16)
        low = (x - high.astype(f32)).astype(bf16)
        return (lax.dot_general(high, hits, dims, preferred_element_type=f32)
                + lax.dot_general(low, hits, dims, preferred_element_type=f32))

    total = summed(last)
    scale = 1.0 / (1.0 + total[48:80])
    for j in (3, 0, 1, 2):
        if j < 3:
            total = summed(row(3 + j))
        for i in range(8):
            n = 8 * j + i
            if n < proj_ref.shape[0]:
                proj_ref[n] = total[fields * i : fields * (i + 1)] * scale[n : n + 1]


def node_constants():
    roots = ((0.5, 1.0, 2.0), (0.0, 1.0, -4.0), (0.0, 0.5, 2.0))
    table = np.zeros((7, 32, LANES), np.float32)
    for n in range(27):
        table[6, n] = 1.0
        for c, i in enumerate((n // 9, n // 3 % 3, n % 3)):
            table[2 * c, n], table[2 * c + 1, n] = roots[i][0], roots[i][1]
            table[6, n] *= roots[i][2]
    return table


def hop(side, straight):
    side = lax.all_to_all(side, "rad", split_axis=0, concat_axis=0, tiled=True)
    back = passed_along(side[:, 0], "lat", -1)
    onward = passed_along(side[:, 1], "lat", 1)
    straight = lax.all_to_all(straight, "rad", split_axis=0, concat_axis=0, tiled=True)
    return back, straight, onward


def per_device(positions, fields, velocity, counts, elements, routes):
    lat_count, rad_count = lax.axis_size("lat"), lax.axis_size("rad")
    lat = lax.axis_index("lat")
    devices = lat_count * rad_count
    blocks = positions.shape[0]
    capacity = max(1, 2 * blocks // (3 * rad_count))
    sheet = rad_count * capacity
    pitch = (capacity + 7) // 8 * 8
    places = 3 * sheet
    order = jnp.arange(blocks, dtype=jnp.int32)
    valid = order < counts[0]
    lat_to = (lat + routes[0] // sheet - 1) % lat_count
    row_of = ((lat_to * rad_count + routes[0] % sheet // capacity) * pitch + routes[0] % capacity).astype(jnp.int32)

    at_row = (row_of[None, :] == jnp.arange(devices * pitch, dtype=jnp.int32)[:, None]) & valid[None, :]
    want = jnp.max(jnp.where(at_row, elements[1][None, :], -1), axis=1)
    route = jnp.max(jnp.where(at_row, routes[1][None, :], -1), axis=1)
    request = jnp.concatenate([want.reshape(devices, pitch), route.reshape(devices, pitch)], axis=1)
    request = lax.all_to_all(request, ("lat", "rad"), split_axis=0, concat_axis=0, tiled=True)
    asked, next_route = request[:, :pitch].reshape(-1), request[:, pitch:].reshape(-1)
    reply = columns_of(velocity, asked).reshape(devices, pitch, LANES)
    reply = lax.all_to_all(reply, ("lat", "rad"), split_axis=0, concat_axis=0, tiled=True)
    reply = reply.reshape(devices * pitch, LANES)

    place = jnp.arange(places, dtype=jnp.int32)
    at_place = (routes[0][None, :] == place[:, None]) & valid[None, :]
    first_source = jnp.min(jnp.where(at_place, order[None, :], blocks), axis=1)
    came = jnp.arange(devices * pitch, dtype=jnp.int32)
    sheet_in = (lat - came // (rad_count * pitch) + 1) % lat_count
    index_in = sheet_in * sheet + came // pitch % rad_count * capacity + came % pitch
    at_place = next_route[None, :] == place[:, None]
    second_source = jnp.min(jnp.where(at_place, index_in[None, :], places), axis=1)

    points = jnp.transpose(positions, (1, 0, 2))
    midway = pl.pallas_call(
        midway_kernel, out_shape=jax.ShapeDtypeStruct(points.shape, f32),
        in_specs=[VM, VM], out_specs=VM, name="midway",
    )(points, columns_of(velocity, elements[0]))

    group_rows = (ROWS * capacity + 7) // 8 * 8
    parcels = [jax.ShapeDtypeStruct((rad_count, 2, group_rows, LANES), f32),
               jax.ShapeDtypeStruct((rad_count, group_rows, LANES), f32)]
    parcels = pl.pallas_call(
        partial(home_kernel, capacity=capacity), out_shape=parcels,
        in_specs=[SM] * 3 + [VM] * 5, out_specs=[VM] * 2, name="home",
        scratch_shapes=[pltpu.VMEM((blocks, LANES), f32), pltpu.VMEM((3, blocks, LANES), f32),
                        pltpu.VMEM((blocks + 1, 8, LANES), f32)],
    )(row_of, first_source, elements[2], points, midway, reply, fields, jnp.asarray(node_constants()))
    parcels = pl.pallas_call(
        partial(middle_kernel, capacity=capacity),
        out_shape=[jax.ShapeDtypeStruct(x.shape, f32) for x in parcels],
        in_specs=[SM] + [VM] * 3, out_specs=[VM] * 2, name="middle",
        scratch_shapes=[pltpu.VMEM((places + 1, 8, LANES), f32)],
    )(second_source, *hop(*parcels))
    moved, projected = pl.pallas_call(
        partial(final_kernel, capacity=capacity),
        out_shape=[jax.ShapeDtypeStruct((3, places, LANES), f32),
                   jax.ShapeDtypeStruct((27, fields.shape[1], velocity.shape[1]), f32)],
        in_specs=[VM] * 3, out_specs=[VM] * 2, name="final",
        scratch_shapes=[pltpu.VMEM((places, 8, LANES), f32)],
    )(*hop(*parcels))
    return jnp.transpose(moved, (1, 0, 2)), projected


def solution(mesh):
    in_specs = (
        P(("lat", "rad"), None, None),
        P(("lat", "rad"), None, None),
        P(None, ("lat", "rad")),
        P(("lat", "rad")),
        P(None, ("lat", "rad")),
        P(None, ("lat", "rad")),
    )
    out_specs = (P(("lat", "rad"), None, None), P(None, None, ("lat", "rad")))

    def body(*args):
        return tuple(per_device(*args))

    return jax.shard_map(
        body, mesh=mesh, in_specs=in_specs, out_specs=out_specs, check_vma=False
    )
```

```python
from functools import partial

import jax
import jax.numpy as jnp
import numpy as np
from jax import lax
from jax.experimental import pallas as pl
from jax.experimental.pallas import tpu as pltpu
from jax.sharding import PartitionSpec as P

time_step = 0.4
exact = lax.Precision.HIGHEST
LANES = 128
ROWS = 7
TAG = 80
VM = pl.BlockSpec(memory_space=pltpu.VMEM)
SM = pl.BlockSpec(memory_space=pltpu.SMEM)
f32 = jnp.float32
bf16 = jnp.bfloat16


def passed_along(x, axis, by):
    size = lax.axis_size(axis)
    return lax.ppermute(x, axis, [(i, (i + by) % size) for i in range(size)])


def lagrange(coord):
    return (
        2.0 * (coord - 0.5) * (coord - 1.0),
        -4.0 * coord * (coord - 1.0),
        2.0 * coord * (coord - 0.5),
    )


def columns_of(velocity, picks):
    owned = velocity.shape[1]
    table = jnp.pad(velocity, ((0, LANES - velocity.shape[0]), (0, 0)))
    chosen = (picks[:, None] == jnp.arange(owned, dtype=jnp.int32)[None, :]).astype(f32)
    return lax.dot_general(chosen, table, (((1,), (1,)), ((), ())), precision=exact)


def eight_speeds(columns, x, y, z):
    lx, ly, lz = lagrange(x), lagrange(y), lagrange(z)
    out = []
    for c in range(3):
        total = None
        for i in range(3):
            plane = None
            for j in range(3):
                base = c * 27 + i * 9 + j * 3
                line = sum(columns[:, base + k : base + k + 1] * lz[k] for k in range(3))
                line = line * ly[j]
                plane = line if plane is None else plane + line
            plane = plane * lx[i]
            total = plane if total is None else total + plane
        out.append(total)
    return out


def midway_kernel(pos_ref, col_ref, out_ref):
    for g in range(pos_ref.shape[1] // 8):
        rows = slice(g * 8, g * 8 + 8)
        x, y, z = (pos_ref[c, rows, :] for c in range(3))
        u = eight_speeds(col_ref[rows, :], x, y, z)
        for c, p in enumerate((x, y, z)):
            out_ref[c, rows, :] = p + (0.5 * time_step) * u[c]


def home_kernel(row_ref, src_ref, e2_ref, pos_ref, mid_ref, reply_ref, fields_ref, const_ref,
                side, straight, cols, land, tiles, *, capacity):
    blocks = pos_ref.shape[1]

    def fetch(g, carry):
        for i in range(8):
            s = g * 8 + i
            cols[pl.ds(s, 1), :] = reply_ref[pl.ds(row_ref[s], 1), :]
        return carry

    lax.fori_loop(0, blocks // 8, fetch, 0)

    for g in range(blocks // 8):
        rows = slice(g * 8, g * 8 + 8)
        x, y, z = (mid_ref[c, rows, :] for c in range(3))
        u = eight_speeds(cols[rows, :], x, y, z)
        for c in range(3):
            land[c, rows, :] = pos_ref[c, rows, :] + time_step * u[c]

    lane = lax.broadcasted_iota(jnp.int32, (8, LANES), 1)
    sub = lax.broadcasted_iota(jnp.int32, (8, LANES), 0)
    own_slot = (lane // 16) == sub
    tag_slot = (lane == TAG) & (sub == 0)

    step = 16 if blocks % 16 == 0 else 8

    def block(g, carry):
        for i in range(step):
            s = g * step + i
            coords = [land[c, pl.ds(s, 1), :] for c in range(3)]
            phi = const_ref[6]
            for c in range(3):
                phi = phi * ((coords[c] - const_ref[2 * c]) * (coords[c] - const_ref[2 * c + 1]))
            high = phi.astype(bf16)
            low = (phi - high.astype(f32)).astype(bf16)
            spread = jnp.concatenate([fields_ref[s]] * 8, axis=0)
            dims = (((1,), (1,)), ((), ()))
            full = lax.dot_general(jnp.concatenate([high, low], axis=1),
                                   jnp.concatenate([spread, spread], axis=1), dims,
                                   preferred_element_type=f32)
            weight = jnp.sum(phi * phi, axis=1, keepdims=True)
            tag = (e2_ref[s] + 1).astype(f32)
            parts = [jnp.where(own_slot, full[8 * j : 8 * j + 8], 0.0) for j in range(4)]
            parts[3] = jnp.where(tag_slot, tag, parts[3])
            for j in range(4):
                parts[3] = jnp.where(lane == sub + (48 + 8 * j), weight[8 * j : 8 * j + 8], parts[3])
            rows = coords + [jnp.sum(part, axis=0, keepdims=True) for part in parts]
            tiles[s, 0:7, :] = jnp.concatenate(rows, axis=0)
        return carry

    lax.fori_loop(0, blocks // step, block, 0)
    tiles[blocks] = jnp.zeros((8, LANES), f32)
    send(src_ref, tiles, side, straight, capacity)


def send(src_ref, tiles, side, straight, capacity):
    rad_count = straight.shape[0]

    def some(q, carry):
        for k in range(3):
            for c in range(capacity):
                tile = tiles[src_ref[(k * rad_count + q) * capacity + c], 0:ROWS, :]
                rows = slice(c * ROWS, (c + 1) * ROWS)
                if k == 1:
                    straight[q, rows, :] = tile
                else:
                    side[q, k // 2, rows, :] = tile
        return carry

    lax.fori_loop(0, rad_count, some, 0)


def collect(ins, tiles, capacity):
    rad_count = ins[0].shape[0]

    def some(q, carry):
        for k, ref in enumerate(ins):
            for c in range(capacity):
                p = (k * rad_count + q) * capacity + c
                tiles[p, 0:ROWS, :] = ref[q, c * ROWS : (c + 1) * ROWS, :]
        return carry

    lax.fori_loop(0, rad_count, some, 0)


def middle_kernel(src_ref, in0, in1, in2, side, straight, tiles, *, capacity):
    collect((in0, in1, in2), tiles, capacity)
    tiles[tiles.shape[0] - 1] = jnp.zeros((8, LANES), f32)
    send(src_ref, tiles, side, straight, capacity)


def final_kernel(in0, in1, in2, moved_ref, proj_ref, tiles, *, capacity):
    places = tiles.shape[0]
    owned = proj_ref.shape[2]
    fields = proj_ref.shape[1]
    collect((in0, in1, in2), tiles, capacity)
    for c in range(3):
        moved_ref[c] = tiles[:, c, :]

    def row(j):
        return tiles[:, j, :]

    last = row(6)
    tag = last[:, TAG : TAG + 1].astype(jnp.int32) - 1
    hits = (tag == lax.broadcasted_iota(jnp.int32, (places, owned), 1)).astype(bf16)
    dims = (((0,), (0,)), ((), ()))

    def summed(x):
        high = x.astype(bf16)
        low = (x - high.astype(f32)).astype(bf16)
        return (lax.dot_general(high, hits, dims, preferred_element_type=f32)
                + lax.dot_general(low, hits, dims, preferred_element_type=f32))

    total = summed(last)
    scale = 1.0 / (1.0 + total[48:80])
    for j in (3, 0, 1, 2):
        if j < 3:
            total = summed(row(3 + j))
        for i in range(8):
            n = 8 * j + i
            if n < proj_ref.shape[0]:
                proj_ref[n] = total[fields * i : fields * (i + 1)] * scale[n : n + 1]


def node_constants():
    roots = ((0.5, 1.0, 2.0), (0.0, 1.0, -4.0), (0.0, 0.5, 2.0))
    table = np.zeros((7, 32, LANES), np.float32)
    for n in range(27):
        table[6, n] = 1.0
        for c, i in enumerate((n // 9, n // 3 % 3, n % 3)):
            table[2 * c, n], table[2 * c + 1, n] = roots[i][0], roots[i][1]
            table[6, n] *= roots[i][2]
    return table


def hop(side, straight):
    side = lax.all_to_all(side, "rad", split_axis=0, concat_axis=0, tiled=True)
    back = passed_along(side[:, 0], "lat", -1)
    onward = passed_along(side[:, 1], "lat", 1)
    straight = lax.all_to_all(straight, "rad", split_axis=0, concat_axis=0, tiled=True)
    return back, straight, onward


def per_device(positions, fields, velocity, counts, elements, routes):
    lat_count, rad_count = lax.axis_size("lat"), lax.axis_size("rad")
    lat = lax.axis_index("lat")
    devices = lat_count * rad_count
    blocks = positions.shape[0]
    capacity = max(1, 2 * blocks // (3 * rad_count))
    sheet = rad_count * capacity
    pitch = (capacity + 7) // 8 * 8
    places = 3 * sheet
    order = jnp.arange(blocks, dtype=jnp.int32)
    valid = order < counts[0]
    lat_to = (lat + routes[0] // sheet - 1) % lat_count
    row_of = ((lat_to * rad_count + routes[0] % sheet // capacity) * pitch + routes[0] % capacity).astype(jnp.int32)

    at_row = (row_of[None, :] == jnp.arange(devices * pitch, dtype=jnp.int32)[:, None]) & valid[None, :]
    want = jnp.max(jnp.where(at_row, elements[1][None, :], -1), axis=1)
    route = jnp.max(jnp.where(at_row, routes[1][None, :], -1), axis=1)
    request = jnp.concatenate([want.reshape(devices, pitch), route.reshape(devices, pitch)], axis=1)
    request = lax.all_to_all(request, ("lat", "rad"), split_axis=0, concat_axis=0, tiled=True)
    asked, next_route = request[:, :pitch].reshape(-1), request[:, pitch:].reshape(-1)
    reply = columns_of(velocity, asked).reshape(devices, pitch, LANES)
    reply = lax.all_to_all(reply, ("lat", "rad"), split_axis=0, concat_axis=0, tiled=True)
    reply = reply.reshape(devices * pitch, LANES)

    place = jnp.arange(places, dtype=jnp.int32)
    at_place = (routes[0][None, :] == place[:, None]) & valid[None, :]
    first_source = jnp.min(jnp.where(at_place, order[None, :], blocks), axis=1)
    came = jnp.arange(devices * pitch, dtype=jnp.int32)
    sheet_in = (lat - came // (rad_count * pitch) + 1) % lat_count
    index_in = sheet_in * sheet + came // pitch % rad_count * capacity + came % pitch
    at_place = next_route[None, :] == place[:, None]
    second_source = jnp.min(jnp.where(at_place, index_in[None, :], places), axis=1)

    points = jnp.transpose(positions, (1, 0, 2))
    midway = pl.pallas_call(
        midway_kernel, out_shape=jax.ShapeDtypeStruct(points.shape, f32),
        in_specs=[VM, VM], out_specs=VM, name="midway",
    )(points, columns_of(velocity, elements[0]))

    group_rows = (ROWS * capacity + 7) // 8 * 8
    parcels = [jax.ShapeDtypeStruct((rad_count, 2, group_rows, LANES), f32),
               jax.ShapeDtypeStruct((rad_count, group_rows, LANES), f32)]
    parcels = pl.pallas_call(
        partial(home_kernel, capacity=capacity), out_shape=parcels,
        in_specs=[SM] * 3 + [VM] * 5, out_specs=[VM] * 2, name="home",
        scratch_shapes=[pltpu.VMEM((blocks, LANES), f32), pltpu.VMEM((3, blocks, LANES), f32),
                        pltpu.VMEM((blocks + 1, 8, LANES), f32)],
    )(row_of, first_source, elements[2], points, midway, reply, fields, jnp.asarray(node_constants()))
    parcels = pl.pallas_call(
        partial(middle_kernel, capacity=capacity),
        out_shape=[jax.ShapeDtypeStruct(x.shape, f32) for x in parcels],
        in_specs=[SM] + [VM] * 3, out_specs=[VM] * 2, name="middle",
        scratch_shapes=[pltpu.VMEM((places + 1, 8, LANES), f32)],
    )(second_source, *hop(*parcels))
    moved, projected = pl.pallas_call(
        partial(final_kernel, capacity=capacity),
        out_shape=[jax.ShapeDtypeStruct((3, places, LANES), f32),
                   jax.ShapeDtypeStruct((27, fields.shape[1], velocity.shape[1]), f32)],
        in_specs=[VM] * 3, out_specs=[VM] * 2, name="final",
        scratch_shapes=[pltpu.VMEM((places, 8, LANES), f32)],
    )(*hop(*parcels))
    return jnp.transpose(moved, (1, 0, 2)), projected


def solution(mesh):
    in_specs = (
        P(("lat", "rad"), None, None),
        P(("lat", "rad"), None, None),
        P(None, ("lat", "rad")),
        P(("lat", "rad")),
        P(None, ("lat", "rad")),
        P(None, ("lat", "rad")),
    )
    out_specs = (P(("lat", "rad"), None, None), P(None, None, ("lat", "rad")))

    def body(*args):
        return tuple(per_device(*args))

    return jax.shard_map(
        body, mesh=mesh, in_specs=in_specs, out_specs=out_specs, check_vma=False
    )
```
